32 devices in a mesh: dp: 4 (over x, core), ctx: 8 (over z, y).
Axes of the slice: x: 2, y: 2, z: 4, core: 2. Of those that a mesh axis runs over, the one named last changes fastest.
Arguments:
- tokens: bfloat16 [4096, 1792], P(('dp', 'ctx')), may hold values from -6 to 6
- cotangent: bfloat16 [4096, 1792], P(('dp', 'ctx')), may hold values from -6 to 6
- expert_ids: int32 [4096, 4], P(('dp', 'ctx')), may hold values from 0 to 15, all different within a row; in each aligned block of 128 rows (0 to 127, 128 to 255, ...) at most 40 rows name the same one
- norm_gain: float32 [1792], replicated, may hold values from 0.5 to 1.5
- router_weight: bfloat16 [1792, 16], replicated, may hold values from -0.125 to 0.125
- gate_weight: bfloat16 [16, 1792, 1536], P('ctx', None, 'dp'), may hold values from -0.125 to 0.125
- up_weight: bfloat16 [16, 1792, 1536], P('ctx', None, 'dp'), may hold values from -0.125 to 0.125
- down_weight: bfloat16 [16, 1536, 1792], P('ctx', 'dp'), may hold values from -0.15625 to 0.15625
Outputs:
- grad_tokens: bfloat16 [4096, 1792], P(('dp', 'ctx'))
- grad_gate: bfloat16 [16, 1792, 1536], P('ctx', None, 'dp')
- grad_up: bfloat16 [16, 1792, 1536], P('ctx', None, 'dp')
- grad_down: bfloat16 [16, 1536, 1792], P('ctx', 'dp')
- grad_router: float32 [1792, 16], P(('dp', 'ctx'))
- grad_gain: float32 [1792], P(('dp', 'ctx'))
The draws below stay inside these ranges and needn't reach their ends.
Inputs may be any that keep to these rules, and one draw needn't show every extreme that they name: `expert_ids`: each row names 4 different experts; among the rows of one device no expert is named more than 40 times.
All inputs are finite; a program needn't handle non-finite values.
Results may differ from the reference program's by a relative error of at most 0.02.
Values may be sent and summed in bfloat16 or wider, within the bound.
A program may use at most 192 MiB of HBM per device.

```python
import math
import jax
import jax.numpy as jnp
import numpy as np
from jax import lax

D = 1792
FF = 1536
TOP = 4
TOK_DEV = 128
EXPERTS = 16
CAP = 40
TOKENS = 4096
N_DP = 4
N_CTX = 8


def raised(values, own_key, source, target, blocks, factor):
    def block_of(dim):
        return (jnp.arange(values.shape[dim]) // (values.shape[dim] // blocks)).reshape((-1,) + (1,) * (values.ndim - 1 - dim))

    near = jax.random.permutation(own_key, blocks)[block_of(target)]
    second = (block_of(target) + blocks // 2) % blocks
    return jnp.where((block_of(source) == near) | (block_of(source) == second), factor * values, values)


def block_scale(stream_key, shape, cuts, smallest, largest):
    gain, own = 1.0, jax.random.fold_in(stream_key, 6)
    for axis_at, shards_of in cuts:
        draws = jnp.exp(jax.random.uniform(jax.random.fold_in(own, axis_at), (shards_of,), jnp.float32, smallest / len(cuts), largest / len(cuts)))
        gain = gain * jnp.repeat(draws, shape[axis_at] // shards_of).reshape([-1 if axis == axis_at else 1 for axis in range(len(shape))])
    return gain


def shared_out(key, own, number, rows, count, top, bound, skew):
    order = jax.random.permutation(key, count)
    crowded, common = load_shares(count, rows * top, bound, skew, True), load_shares(count, rows * top, bound, skew, False)
    places = jnp.arange(count)

    def named(lengths, rotation):
        used = int((lengths > 0).sum())
        fixed = max(1, used // 4)
        moved = fixed + (places - fixed + rotation * (used - fixed)) % max(1, count - fixed)
        return jnp.zeros((count,), jnp.int32).at[order[jnp.where(places < fixed, places, moved)]].set(jnp.asarray(lengths, jnp.int32))

    lengths = jnp.where(number % 4 == 0, named(crowded, number // 4), named(common, number - number // 4 - 1))
    mixed = jax.random.permutation(jax.random.fold_in(own, 3), count)
    donor, taker = mixed[0:count // 2 * 2:2], mixed[1:count // 2 * 2:2]
    room = jnp.minimum(lengths[donor] - 1, bound - lengths[taker]) // 2
    room = jnp.where((donor == order[0]) | (taker == order[0]) | (lengths[taker] == 0), 0, jnp.maximum(room, 0))
    moved = jax.random.randint(jax.random.fold_in(own, 4), (count // 2,), 0, 1 << 20) % (room + 1)
    lengths = lengths.at[donor].add(-moved).at[taker].add(moved)
    items = jnp.searchsorted(jnp.cumsum(lengths), jnp.arange(rows * top), side="right").astype(jnp.int32)
    table = items.reshape(top, rows).T
    table = table[jax.random.permutation(jax.random.fold_in(own, 1), rows)]
    rotation = jax.random.randint(jax.random.fold_in(own, 2), (rows, 1), 0, top)
    return jnp.take_along_axis(table, (jnp.arange(top)[None, :] + rotation) % top, axis=1)


def load_shares(number_of, total, limit, lean, full):
    portions = [(1 << 20) // math.isqrt(rank ** lean) + 1 for rank in range(1, number_of + 1)]
    largest = limit if full else min(limit, max(-(-total // number_of), total * portions[0] // sum(portions)))
    least = 1 if total - largest >= number_of - 1 else 0
    counts, spare = [largest] + [least] * (number_of - 1), total - largest - least * (number_of - 1)
    while spare > 0:
        free = [i for i in range(1, number_of) if counts[i] < largest] or [i for i in range(1, number_of) if counts[i] < limit]
        pool, budget = sum([portions[i] for i in free]), spare
        for i in free:
            extra = min(limit - counts[i], max(1, budget * portions[i] // pool), spare)
            counts[i] = counts[i] + extra
            spare = spare - extra
    return np.array(counts)


def bell_draw(own_key, shape, width, most, pieces=(), held_as=jnp.bfloat16):
    gain = block_scale(own_key, shape, pieces, -0.22, 0.18) if pieces else 1.0
    result = jax.random.normal(own_key, shape, jnp.float32) * width * gain
    return jnp.minimum(jnp.maximum(result, -most), most).astype(held_as)


def gaussian_with(stream_key, shape, spread, limit, pieces, heavy, kind=jnp.bfloat16):
    values = spread * jax.random.normal(stream_key, shape, jnp.float32)
    if pieces:
        values = values * block_scale(stream_key, shape, pieces, -0.22, 0.18)
    return jnp.clip(raised(values, jax.random.fold_in(stream_key, 3), *heavy), -limit, limit).astype(kind)


def setup_inputs(seed: int = 0) -> dict:
    keys = jax.random.split(jax.random.key(seed), 9)
    tokens = gaussian_with(keys[0], (TOKENS, D), 1.0, 6.0, ((0, 32),), (0, 1, 32, 2.75))
    cotangent = bell_draw(keys[1], (TOKENS, D), 1.0, 6.0, ((0, 32),))
    expert_ids_keys = jax.random.split(jax.random.fold_in(keys[2], 1), TOKENS // TOK_DEV)
    expert_ids_turns = jax.random.permutation(jax.random.fold_in(keys[2], 3), TOKENS // TOK_DEV)
    expert_ids = jax.vmap(lambda own, number: shared_out(jax.random.fold_in(keys[2], 2), own, number, TOK_DEV, EXPERTS, TOP, CAP, 2))(expert_ids_keys, expert_ids_turns).reshape((TOKENS, TOP))
    norm_gain = jnp.clip(1.0 + 0.1 * jax.random.normal(keys[3], (D,), jnp.float32), 0.5, 1.5)
    router_weight = bell_draw(keys[4], (D, EXPERTS), D ** -0.5, 0.125)
    gate_weight = bell_draw(keys[5], (EXPERTS, D, FF), D ** -0.5, 0.125, ((0, 8), (2, 4)))
    up_weight = bell_draw(keys[6], (EXPERTS, D, FF), D ** -0.5, 0.125, ((0, 8), (2, 4)))
    down_weight = bell_draw(keys[7], (EXPERTS, FF, D), FF ** -0.5, 0.15625, ((0, 8), (1, 4)))
    return dict(tokens=tokens, cotangent=cotangent, expert_ids=expert_ids, norm_gain=norm_gain, router_weight=router_weight, gate_weight=gate_weight, up_weight=up_weight, down_weight=down_weight)


EPSILON = 1e-05
SWISH_SCALE = 1.702

def reference(tokens, cotangent, expert_ids, norm_gain, router_weight, gate_weight, up_weight, down_weight):
    ntoken = tokens.shape[0]
    widened = tokens.astype(jnp.float32)
    inverse = lax.rsqrt(lax.optimization_barrier(jnp.mean(widened * widened, axis=1, keepdims=True)) + EPSILON)
    scaled = widened * inverse
    normed = (scaled * norm_gain).astype(jnp.bfloat16)
    logits = jnp.dot(normed, router_weight, preferred_element_type=jnp.float32)
    chosen = jnp.take_along_axis(logits, expert_ids, axis=1)
    lifted = jnp.exp(chosen)
    gates = lifted / lax.optimization_barrier(jnp.sum(lifted, axis=1, keepdims=True))
    devices = N_DP * N_CTX
    per_device = TOK_DEV * TOP
    block_ids = expert_ids.reshape(devices, per_device)
    labels = jnp.arange(EXPERTS, dtype=jnp.int32)
    hits = (block_ids[:, :, None] == labels).astype(jnp.int32)
    rank = lax.optimization_barrier(jnp.sum((jnp.cumsum(hits, axis=1) - 1) * hits, axis=2))
    position = jnp.arange(devices, dtype=jnp.int32)[:, None] * CAP + rank
    assign = jnp.arange(devices * per_device, dtype=jnp.int32)
    flat_ids = block_ids.reshape(-1)
    flat_pos = position.reshape(-1).astype(jnp.int32)
    table = jnp.zeros((EXPERTS, devices * CAP), jnp.int32).at[flat_ids, flat_pos].set(assign)
    present_all = jnp.zeros((EXPERTS, devices * CAP), jnp.float32).at[flat_ids, flat_pos].set(1.0)
    gates_flat = gates.reshape(-1)

    def expert_step(carry, inputs):
        grad_tok, score_acc = carry
        entry, present, w_gate, w_up, w_down = inputs
        token = entry // TOP
        keep = present[:, None] > 0.0
        rows = jnp.where(keep, normed[token], jnp.zeros_like(normed[token]))
        upstream = jnp.where(keep, cotangent[token], jnp.zeros_like(cotangent[token]))
        weight = present * gates_flat[entry]
        gate_pre = jnp.dot(rows, w_gate, preferred_element_type=jnp.float32)
        up_pre = jnp.dot(rows, w_up, preferred_element_type=jnp.float32)
        squash = jax.nn.sigmoid(SWISH_SCALE * gate_pre)
        hidden = (gate_pre * squash * (up_pre + 1.0)).astype(jnp.bfloat16)
        grad_out = jnp.dot(upstream, w_down.T, preferred_element_type=jnp.float32)
        score = lax.optimization_barrier(jnp.sum(grad_out * hidden.astype(jnp.float32), axis=1))
        grad_hidden = weight[:, None] * grad_out
        slope = squash + SWISH_SCALE * gate_pre * squash * (1.0 - squash)
        grad_pre_gate = (grad_hidden * (up_pre + 1.0) * slope).astype(jnp.bfloat16)
        grad_pre_up = (grad_hidden * gate_pre * squash).astype(jnp.bfloat16)
        scaled_up = (weight[:, None] * upstream.astype(jnp.float32)).astype(jnp.bfloat16)
        down_grad = jnp.dot(hidden.T, scaled_up, preferred_element_type=jnp.float32).astype(jnp.bfloat16)
        gate_grad = jnp.dot(rows.T, grad_pre_gate, preferred_element_type=jnp.float32).astype(jnp.bfloat16)
        up_grad = jnp.dot(rows.T, grad_pre_up, preferred_element_type=jnp.float32).astype(jnp.bfloat16)
        back = jnp.dot(grad_pre_gate, w_gate.T, preferred_element_type=jnp.float32)
        back = back + jnp.dot(grad_pre_up, w_up.T, preferred_element_type=jnp.float32)
        grad_tok = grad_tok.at[token].add(back)
        score_acc = score_acc.at[entry].add(score * present)
        return ((grad_tok, score_acc), (gate_grad, up_grad, down_grad))
    start = (jnp.zeros((ntoken, D), jnp.float32), jnp.zeros((ntoken * TOP,), jnp.float32))
    (grad_tok, score_acc), (grad_gate, grad_up, grad_down) = lax.scan(expert_step, start, (table, present_all, gate_weight, up_weight, down_weight))
    score_tok = score_acc.reshape(ntoken, TOP)
    mixed = lax.optimization_barrier(jnp.sum(gates * score_tok, axis=1, keepdims=True))
    grad_chosen = gates * (score_tok - mixed)
    member = expert_ids[:, :, None] == labels
    grad_logits = lax.optimization_barrier(jnp.sum(jnp.where(member, grad_chosen[:, :, None], 0.0), axis=1)).astype(jnp.bfloat16)
    grad_normed = grad_tok + jnp.dot(grad_logits, router_weight.T, preferred_element_type=jnp.float32)
    grad_router = jnp.dot(normed.T, grad_logits, preferred_element_type=jnp.float32)
    grad_gain = lax.optimization_barrier(jnp.sum(grad_normed * scaled, axis=0))
    grad_scaled = grad_normed * norm_gain
    correction = lax.optimization_barrier(jnp.mean(grad_scaled * scaled, axis=1, keepdims=True))
    grad_tokens = (cotangent.astype(jnp.float32) + inverse * (grad_scaled - scaled * correction)).astype(jnp.bfloat16)
    return (grad_tokens, grad_gate, grad_up, grad_down, grad_router, grad_gain)
```

```python
import functools

import jax
import jax.numpy as jnp
from jax import lax
from jax.experimental import pallas as pl
from jax.experimental.pallas import tpu as pltpu
from jax.sharding import PartitionSpec as P

EPSILON = 1e-05
SWISH_SCALE = 1.702
MESH = pl.DeviceIdType.MESH
ANY = pl.BlockSpec(memory_space=pl.ANY)
VMEM = pl.BlockSpec(memory_space=pltpu.VMEM)


def greet_all(n_dp, n_ctx):
    n = n_dp * n_ctx
    me = lax.axis_index("dp") * n_ctx + lax.axis_index("ctx")
    barrier = pltpu.get_barrier_semaphore()

    def hello(i, carry):
        peer = lax.rem(me + i, n)
        pl.semaphore_signal(
            barrier,
            inc=1,
            device_id=(lax.div(peer, n_ctx), lax.rem(peer, n_ctx)),
            device_id_type=MESH,
        )
        return carry

    lax.fori_loop(1, n, hello, 0)
    pl.semaphore_wait(barrier, n - 1)


def spread_copy(n_dp, n_ctx, i, src_of, land, send_sem, recv_sem, sending):
    n = n_dp * n_ctx
    me = lax.axis_index("dp") * n_ctx + lax.axis_index("ctx")
    peer = lax.rem(me + i, n)
    source = me if sending else lax.rem(me + n - i, n)
    return pltpu.make_async_remote_copy(
        src_ref=src_of(peer),
        dst_ref=land.at[source],
        send_sem=send_sem.at[i],
        recv_sem=recv_sem.at[i],
        device_id=(lax.div(peer, n_ctx), lax.rem(peer, n_ctx)),
        device_id_type=MESH,
    )


def exchange_kernel(n_dp, n_ctx, keep, x_ref, o_ref, land, send_sem, recv_sem):
    n = n_dp * n_ctx
    me = lax.axis_index("dp") * n_ctx + lax.axis_index("ctx")
    greet_all(n_dp, n_ctx)
    src_of = lambda peer: x_ref.at[peer]

    def start(i, carry):
        spread_copy(n_dp, n_ctx, i, src_of, land, send_sem, recv_sem, True).start()
        return carry

    lax.fori_loop(1, n, start, 0)
    land[pl.ds(me, 1)] = x_ref[pl.ds(me, 1)]

    def finish(i, carry):
        spread_copy(n_dp, n_ctx, i, src_of, land, send_sem, recv_sem, True).wait_send()
        spread_copy(n_dp, n_ctx, i, src_of, land, send_sem, recv_sem, False).wait_recv()
        return carry

    lax.fori_loop(1, n, finish, 0)
    o_ref[...] = jnp.sum(land[...].reshape(n // keep, keep, 8, 128), axis=0)


def exchange(x, n_dp, n_ctx, keep, cid):
    n = n_dp * n_ctx
    return pl.pallas_call(
        functools.partial(exchange_kernel, n_dp, n_ctx, keep),
        out_shape=jax.ShapeDtypeStruct((keep, 8, 128), jnp.float32),
        in_specs=[VMEM],
        out_specs=VMEM,
        scratch_shapes=[
            pltpu.VMEM((n, 8, 128), jnp.float32),
            pltpu.SemaphoreType.DMA((n,)),
            pltpu.SemaphoreType.DMA((n,)),
        ],
        compiler_params=pltpu.CompilerParams(collective_id=cid, has_side_effects=True),
    )(x)


def dispatch_kernel(
    n_dp, n_ctx, rows_ref, grad_ref, gate_ref, out_rows, out_grad, out_gate,
    own, own_sem, gate_send, gate_recv, ring_send, ring_recv, far_send, far_recv, sib_send, sib_recv,
):
    n = n_dp * n_ctx
    d, c = lax.axis_index("dp"), lax.axis_index("ctx")
    me = d * n_ctx + c
    far = lax.rem(d + 2, n_dp)
    sib = d + 1 - 2 * lax.rem(d, 2)
    far_sib = lax.rem(sib + 2, n_dp)
    greet_all(n_dp, n_ctx)
    gate_src = lambda peer: gate_ref.at[lax.rem(peer, n_ctx)]
    ins, outs = (rows_ref, grad_ref), (out_rows, out_grad)

    def gate_start(i, carry):
        spread_copy(n_dp, n_ctx, i, gate_src, out_gate, gate_send, gate_recv, True).start()
        return carry

    lax.fori_loop(1, n, gate_start, 0)

    def ring(a, k, sending):
        peer = lax.rem(c + k, n_ctx)
        owner = c if sending else lax.rem(c + n_ctx - k, n_ctx)
        return pltpu.make_async_remote_copy(
            src_ref=ins[a].at[peer],
            dst_ref=outs[a].at[:, d * n_ctx + owner],
            send_sem=ring_send.at[a, k],
            recv_sem=ring_recv.at[a, k],
            device_id=(d, peer),
            device_id_type=MESH,
        )

    def forward(a, k, src, slot, to, send_sem, recv_sem, index):
        return pltpu.make_async_remote_copy(
            src_ref=src,
            dst_ref=outs[a].at[:, slot],
            send_sem=send_sem.at[a, index],
            recv_sem=recv_sem.at[a, index],
            device_id=(to, c),
            device_id_type=MESH,
        )

    def held(a, row, k):
        owner = lax.rem(c + n_ctx - k, n_ctx)
        slot = row * n_ctx + owner
        return slot, (outs[a].at[:, slot])

    loads = []
    for a in range(2):
        load = pltpu.make_async_copy(ins[a].at[c], own.at[a], own_sem.at[a])
        load.start()
        loads.append(load)
        for k in range(1, n_ctx):
            ring(a, k, True).start()
    stores = []
    for a in range(2):
        loads[a].wait()
        store = pltpu.make_async_copy(own.at[a], outs[a].at[:, me], own_sem.at[a])
        store.start()
        stores.append(store)
    out_gate[pl.ds(me, 1)] = gate_ref[pl.ds(c, 1)]

    def pass_far(a, k, wait):
        slot, here = held(a, d, k)
        src = ins[a].at[c] if k == 0 else here
        for copy in (
            forward(a, k, src, slot, far, far_send, far_recv, k),
            forward(a, k, src, slot, sib, sib_send, sib_recv, k),
        ):
            copy.wait_send() if wait else copy.start()

    def pass_sib(a, k, wait):
        slot, here = held(a, far, k)
        copy = forward(a, k, here, slot, sib, sib_send, sib_recv, n_ctx + k)
        copy.wait_send() if wait else copy.start()

    def await_far(a, k):
        slot, here = held(a, far, k)
        forward(a, k, here, slot, far, far_send, far_recv, k).wait_recv()

    lag = 2
    for step in range(2 * n_ctx + lag):
        a, k = divmod(step, n_ctx)
        if step < 2 * n_ctx:
            if k > 0:
                ring(a, k, False).wait_recv()
            pass_far(a, k, False)
        if step >= lag:
            a, k = divmod(step - lag, n_ctx)
            await_far(a, k)
            pass_sib(a, k, False)
    for a in range(2):
        for k in range(n_ctx):
            slot, here = held(a, sib, k)
            forward(a, k, here, slot, sib, sib_send, sib_recv, k).wait_recv()
            slot, here = held(a, far_sib, k)
            forward(a, k, here, slot, sib, sib_send, sib_recv, n_ctx + k).wait_recv()
    for a in range(2):
        stores[a].wait()
        for k in range(n_ctx):
            if k > 0:
                ring(a, k, True).wait_send()
            pass_far(a, k, True)
            pass_sib(a, k, True)

    def gate_finish(i, carry):
        spread_copy(n_dp, n_ctx, i, gate_src, out_gate, gate_send, gate_recv, True).wait_send()
        spread_copy(n_dp, n_ctx, i, gate_src, out_gate, gate_send, gate_recv, False).wait_recv()
        return carry

    lax.fori_loop(1, n, gate_finish, 0)


def dispatch_rows(rows, grad, gate, n_dp, n_ctx):
    n = n_dp * n_ctx
    _, local, cap, width = rows.shape
    arrived = jax.ShapeDtypeStruct((local, n, cap, width), rows.dtype)
    return pl.pallas_call(
        functools.partial(dispatch_kernel, n_dp, n_ctx),
        out_shape=(arrived, arrived, jax.ShapeDtypeStruct((n, 8, 128), jnp.float32)),
        in_specs=[ANY, ANY, VMEM],
        out_specs=(ANY, ANY, VMEM),
        scratch_shapes=[
            pltpu.VMEM((2, local, cap, width), rows.dtype),
            pltpu.SemaphoreType.DMA((2,)),
            pltpu.SemaphoreType.DMA((n,)),
            pltpu.SemaphoreType.DMA((n,)),
            pltpu.SemaphoreType.DMA((2, n_ctx)),
            pltpu.SemaphoreType.DMA((2, n_ctx)),
            pltpu.SemaphoreType.DMA((2, n_ctx)),
            pltpu.SemaphoreType.DMA((2, n_ctx)),
            pltpu.SemaphoreType.DMA((2, 2 * n_ctx)),
            pltpu.SemaphoreType.DMA((2, 2 * n_ctx)),
        ],
        compiler_params=pltpu.CompilerParams(collective_id=0, has_side_effects=True),
    )(rows, grad, gate)


def return_kernel(
    n_dp, n_ctx, back_ref, out_ref,
    mine, sib_land, far_out, far_land, done,
    mine_sem, sib_send, sib_recv, far_send, far_recv, ring_send, ring_recv, own_sem,
):
    d, c = lax.axis_index("dp"), lax.axis_index("ctx")
    far = lax.rem(d + 2, n_dp)
    sib = d + 1 - 2 * lax.rem(d, 2)
    far_sib = lax.rem(sib + 2, n_dp)
    greet_all(n_dp, n_ctx)

    def dest(k):
        return lax.rem(c + k, n_ctx)

    def to_sib(k, which):
        row = far_sib if which == 0 else sib
        return pltpu.make_async_remote_copy(
            src_ref=back_ref.at[:, row * n_ctx + dest(k)],
            dst_ref=sib_land.at[k, which],
            send_sem=sib_send.at[k, which],
            recv_sem=sib_recv.at[k, which],
            device_id=(sib, c),
            device_id_type=MESH,
        )

    def load(k, which):
        row = far if which == 0 else d
        return pltpu.make_async_copy(
            back_ref.at[:, row * n_ctx + dest(k)], mine.at[k, which], mine_sem.at[k, which]
        )

    def to_far(k):
        return pltpu.make_async_remote_copy(
            src_ref=far_out.at[k],
            dst_ref=far_land.at[k],
            send_sem=far_send.at[k],
            recv_sem=far_recv.at[k],
            device_id=(far, c),
            device_id_type=MESH,
        )

    def ring(k, sending):
        owner = c if sending else lax.rem(c + n_ctx - k, n_ctx)
        return pltpu.make_async_remote_copy(
            src_ref=done.at[k],
            dst_ref=out_ref.at[owner],
            send_sem=ring_send.at[k],
            recv_sem=ring_recv.at[k],
            device_id=(d, dest(k)),
            device_id_type=MESH,
        )

    order = list(range(1, n_ctx)) + [0]
    for k in order:
        for which in range(2):
            to_sib(k, which).start()
            load(k, which).start()
    for k in order:
        to_sib(k, 0).wait_recv()
        load(k, 0).wait()
        far_out[k] = (
            mine[k, 0].astype(jnp.float32) + sib_land[k, 0].astype(jnp.float32)
        ).astype(jnp.bfloat16)
        to_far(k).start()
    for k in order:
        to_sib(k, 1).wait_recv()
        load(k, 1).wait()
        to_far(k).wait_recv()
        done[k] = (
            mine[k, 1].astype(jnp.float32)
            + sib_land[k, 1].astype(jnp.float32)
            + far_land[k].astype(jnp.float32)
        ).astype(jnp.bfloat16)
        if k > 0:
            ring(k, True).start()
    own = pltpu.make_async_copy(done.at[0], out_ref.at[c], own_sem)
    own.start()
    own.wait()
    for k in order:
        to_sib(k, 0).wait_send()
        to_sib(k, 1).wait_send()
        to_far(k).wait_send()
        if k > 0:
            ring(k, True).wait_send()
            ring(k, False).wait_recv()


def return_rows(back, n_dp, n_ctx):
    local, n, cap, width = back.shape
    block = (local, cap, width)
    return pl.pallas_call(
        functools.partial(return_kernel, n_dp, n_ctx),
        out_shape=jax.ShapeDtypeStruct((n_ctx,) + block, back.dtype),
        in_specs=[ANY],
        out_specs=ANY,
        scratch_shapes=[
            pltpu.VMEM((n_ctx, 2) + block, back.dtype),
            pltpu.VMEM((n_ctx, 2) + block, back.dtype),
            pltpu.VMEM((n_ctx,) + block, back.dtype),
            pltpu.VMEM((n_ctx,) + block, back.dtype),
            pltpu.VMEM((n_ctx,) + block, back.dtype),
            pltpu.SemaphoreType.DMA((n_ctx, 2)),
            pltpu.SemaphoreType.DMA((n_ctx, 2)),
            pltpu.SemaphoreType.DMA((n_ctx, 2)),
            pltpu.SemaphoreType.DMA((n_ctx,)),
            pltpu.SemaphoreType.DMA((n_ctx,)),
            pltpu.SemaphoreType.DMA((n_ctx,)),
            pltpu.SemaphoreType.DMA((n_ctx,)),
            pltpu.SemaphoreType.DMA,
        ],
        compiler_params=pltpu.CompilerParams(
            collective_id=1, has_side_effects=True, vmem_limit_bytes=48 * 1024 * 1024
        ),
    )(back)


def expert_pass(rows, upstream, weight, gate_weight, up_weight, down_weight):
    gate_pre = jnp.einsum("prd,pdf->prf", rows, gate_weight, preferred_element_type=jnp.float32)
    up_pre = jnp.einsum("prd,pdf->prf", rows, up_weight, preferred_element_type=jnp.float32)
    squash = jax.nn.sigmoid(SWISH_SCALE * gate_pre)
    hidden = (gate_pre * squash * (up_pre + 1.0)).astype(jnp.bfloat16)
    grad_out = jnp.einsum("prd,pfd->prf", upstream, down_weight, preferred_element_type=jnp.float32)
    score = jnp.sum(grad_out * hidden.astype(jnp.float32), axis=2)
    grad_hidden = weight[:, :, None] * grad_out
    slope = squash + SWISH_SCALE * gate_pre * squash * (1.0 - squash)
    grad_pre_gate = (grad_hidden * (up_pre + 1.0) * slope).astype(jnp.bfloat16)
    grad_pre_up = (grad_hidden * gate_pre * squash).astype(jnp.bfloat16)
    scaled_up = (weight[:, :, None] * upstream.astype(jnp.float32)).astype(jnp.bfloat16)
    down_grad = jnp.einsum(
        "prf,prd->pfd", hidden, scaled_up, preferred_element_type=jnp.float32
    ).astype(jnp.bfloat16)
    gate_grad = jnp.einsum(
        "prd,prf->pdf", rows, grad_pre_gate, preferred_element_type=jnp.float32
    ).astype(jnp.bfloat16)
    up_grad = jnp.einsum(
        "prd,prf->pdf", rows, grad_pre_up, preferred_element_type=jnp.float32
    ).astype(jnp.bfloat16)
    back = jnp.einsum(
        "prf,pdf->prd", grad_pre_gate, gate_weight, preferred_element_type=jnp.float32
    )
    back = back + jnp.einsum(
        "prf,pdf->prd", grad_pre_up, up_weight, preferred_element_type=jnp.float32
    )
    return (gate_grad, up_grad, down_grad, back, score)


def tiles(x):
    return jnp.pad(x, ((0, 0), (0, 1024 - x.shape[1]))).reshape(x.shape[0], 8, 128)


def body(
    tokens, cotangent, expert_ids, norm_gain, router_weight, gate_weight, up_weight, down_weight
):
    n_ctx = lax.axis_size("ctx")
    n_dp = lax.axis_size("dp")
    n = n_dp * n_ctx
    local = gate_weight.shape[0]
    experts = router_weight.shape[1]
    rows_here = tokens.shape[0]
    picks = expert_ids.shape[1]
    width = tokens.shape[1]
    assigned = rows_here * picks
    capacity = max(2, rows_here * picks * 5 // (4 * experts))
    capacity = -(-capacity // 8) * 8
    slots = experts * capacity
    widened = tokens.astype(jnp.float32)
    inverse = lax.rsqrt(jnp.mean(widened * widened, axis=1, keepdims=True) + EPSILON)
    scaled = widened * inverse
    normed = (scaled * norm_gain).astype(jnp.bfloat16)
    logits = jnp.dot(normed, router_weight, preferred_element_type=jnp.float32)
    labels = jnp.arange(experts, dtype=jnp.int32)
    member = expert_ids[:, :, None] == labels
    chosen = jnp.sum(jnp.where(member, logits[:, None, :], 0.0), axis=2)
    lifted = jnp.exp(chosen)
    gates = lifted / jnp.sum(lifted, axis=1, keepdims=True)
    hits = member.reshape(assigned, experts).astype(jnp.int32)
    rank = jnp.sum((jnp.cumsum(hits, axis=0) - 1) * hits, axis=1)
    position = expert_ids.reshape(-1) * capacity + rank
    match = (jnp.arange(slots, dtype=jnp.int32)[:, None] == position[None, :]).astype(jnp.float32)
    dispatch = jnp.sum(match.reshape(slots, rows_here, picks), axis=2)
    dispatch_low = dispatch.astype(jnp.bfloat16)
    out_rows = jnp.dot(dispatch_low, normed, preferred_element_type=jnp.float32).astype(
        jnp.bfloat16
    )
    out_rows = out_rows.reshape(n_ctx, local, capacity, width)
    out_grad = jnp.dot(dispatch_low, cotangent, preferred_element_type=jnp.float32).astype(
        jnp.bfloat16
    )
    out_grad = out_grad.reshape(n_ctx, local, capacity, width)
    out_gate = jnp.dot(match, gates.reshape(-1), precision=lax.Precision.HIGHEST)
    out_gate = tiles(out_gate.reshape(n_ctx, local * capacity))
    rows, upstream, weight = dispatch_rows(out_rows, out_grad, out_gate, n_dp, n_ctx)
    rows = rows.reshape(local, n * capacity, width)
    upstream = upstream.reshape(local, n * capacity, width)
    weight = weight.reshape(n, 1024)[:, : local * capacity].reshape(n, local, capacity)
    weight = weight.transpose(1, 0, 2).reshape(local, n * capacity)
    gate_grad, up_grad, down_grad, back, score = expert_pass(
        rows, upstream, weight, gate_weight, up_weight, down_weight
    )
    score_out = score.reshape(local, n, capacity).transpose(1, 0, 2).reshape(n, local * capacity)
    score_slots = exchange(tiles(score_out), n_dp, n_ctx, n_ctx, 2)
    back_slots = return_rows(
        back.astype(jnp.bfloat16).reshape(local, n, capacity, width), n_dp, n_ctx
    )
    back_flat = back_slots.reshape(slots, width)
    score_flat = score_slots.reshape(n_ctx, 1024)[:, : local * capacity].reshape(slots)
    grad_tok = jnp.dot(dispatch_low.T, back_flat, preferred_element_type=jnp.float32)
    score_tok = jnp.dot(score_flat, match, precision=lax.Precision.HIGHEST).reshape(
        rows_here, picks
    )
    mixed = jnp.sum(gates * score_tok, axis=1, keepdims=True)
    grad_chosen = gates * (score_tok - mixed)
    grad_logits = jnp.sum(jnp.where(member, grad_chosen[:, :, None], 0.0), axis=1).astype(
        jnp.bfloat16
    )
    grad_normed = grad_tok + jnp.dot(
        grad_logits, router_weight.T, preferred_element_type=jnp.float32
    )
    router_part = jnp.dot(normed.T, grad_logits, preferred_element_type=jnp.float32)
    gain_part = jnp.sum(grad_normed * scaled, axis=0)
    share = width // n
    parts = jnp.concatenate(
        [router_part.reshape(n, share * experts), gain_part.reshape(n, share)], axis=1
    )
    sums = exchange(tiles(parts), n_dp, n_ctx, 1, 3).reshape(1024)
    router_grad = sums[: share * experts].reshape(share, experts)
    gain_grad = sums[share * experts : share * experts + share]
    grad_scaled = grad_normed * norm_gain
    correction = jnp.mean(grad_scaled * scaled, axis=1, keepdims=True)
    grad_input = (
        cotangent.astype(jnp.float32) + inverse * (grad_scaled - scaled * correction)
    ).astype(jnp.bfloat16)
    return (grad_input, gate_grad, up_grad, down_grad, router_grad, gain_grad)


def solution(mesh):
    return jax.shard_map(
        body,
        mesh=mesh,
        in_specs=(
            P(("dp", "ctx"), None),
            P(("dp", "ctx"), None),
            P(("dp", "ctx"), None),
            P(),
            P(),
            P("ctx", None, "dp"),
            P("ctx", None, "dp"),
            P("ctx", "dp", None),
        ),
        out_specs=(
            P(("dp", "ctx"), None),
            P("ctx", None, "dp"),
            P("ctx", None, "dp"),
            P("ctx", "dp", None),
            P(("dp", "ctx"), None),
            P(("dp", "ctx")),
        ),
        check_vma=False,
    )
```

```python
import functools

import jax
import jax.numpy as jnp
from jax import lax
from jax.experimental import pallas as pl
from jax.experimental.pallas import tpu as pltpu
from jax.sharding import PartitionSpec as P

EPSILON = 1e-05
SWISH_SCALE = 1.702
MESH = pl.DeviceIdType.MESH
ANY = pl.BlockSpec(memory_space=pl.ANY)
VMEM = pl.BlockSpec(memory_space=pltpu.VMEM)


def greet_all(n_dp, n_ctx):
    n = n_dp * n_ctx
    me = lax.axis_index("dp") * n_ctx + lax.axis_index("ctx")
    barrier = pltpu.get_barrier_semaphore()

    def hello(i, carry):
        peer = lax.rem(me + i, n)
        pl.semaphore_signal(
            barrier,
            inc=1,
            device_id=(lax.div(peer, n_ctx), lax.rem(peer, n_ctx)),
            device_id_type=MESH,
        )
        return carry

    lax.fori_loop(1, n, hello, 0)
    pl.semaphore_wait(barrier, n - 1)


def spread_copy(n_dp, n_ctx, i, src_of, land, send_sem, recv_sem, sending):
    n = n_dp * n_ctx
    me = lax.axis_index("dp") * n_ctx + lax.axis_index("ctx")
    peer = lax.rem(me + i, n)
    source = me if sending else lax.rem(me + n - i, n)
    return pltpu.make_async_remote_copy(
        src_ref=src_of(peer),
        dst_ref=land.at[source],
        send_sem=send_sem.at[i],
        recv_sem=recv_sem.at[i],
        device_id=(lax.div(peer, n_ctx), lax.rem(peer, n_ctx)),
        device_id_type=MESH,
    )


def exchange_kernel(n_dp, n_ctx, keep, x_ref, o_ref, land, send_sem, recv_sem):
    n = n_dp * n_ctx
    me = lax.axis_index("dp") * n_ctx + lax.axis_index("ctx")
    greet_all(n_dp, n_ctx)
    src_of = lambda peer: x_ref.at[peer]

    def start(i, carry):
        spread_copy(n_dp, n_ctx, i, src_of, land, send_sem, recv_sem, True).start()
        return carry

    lax.fori_loop(1, n, start, 0)
    land[pl.ds(me, 1)] = x_ref[pl.ds(me, 1)]

    def finish(i, carry):
        spread_copy(n_dp, n_ctx, i, src_of, land, send_sem, recv_sem, True).wait_send()
        spread_copy(n_dp, n_ctx, i, src_of, land, send_sem, recv_sem, False).wait_recv()
        return carry

    lax.fori_loop(1, n, finish, 0)
    o_ref[...] = jnp.sum(land[...].reshape(n // keep, keep, 8, 128), axis=0)


def exchange(x, n_dp, n_ctx, keep, cid):
    n = n_dp * n_ctx
    return pl.pallas_call(
        functools.partial(exchange_kernel, n_dp, n_ctx, keep),
        out_shape=jax.ShapeDtypeStruct((keep, 8, 128), jnp.float32),
        in_specs=[VMEM],
        out_specs=VMEM,
        scratch_shapes=[
            pltpu.VMEM((n, 8, 128), jnp.float32),
            pltpu.SemaphoreType.DMA((n,)),
            pltpu.SemaphoreType.DMA((n,)),
        ],
        compiler_params=pltpu.CompilerParams(collective_id=cid, has_side_effects=True),
    )(x)


def dispatch_kernel(
    n_dp, n_ctx, cap, rows_ref, grad_ref, gate_ref, wg_ref, wu_ref, wd_ref,
    out_rows, out_grad, out_gate, out_pre_g, out_pre_u, out_down,
    own, weights, down_held, chunk, pre, own_sem, weight_sem, chunk_sem, pre_sem,
    gate_send, gate_recv, ring_send, ring_recv, far_send, far_recv, sib_send, sib_recv,
):
    n = n_dp * n_ctx
    local = rows_ref.shape[1]
    span = n_ctx * cap
    chunks = local * n_dp
    d, c = lax.axis_index("dp"), lax.axis_index("ctx")
    me = d * n_ctx + c
    far = lax.rem(d + 2, n_dp)
    sib = d + 1 - 2 * lax.rem(d, 2)
    far_sib = lax.rem(sib + 2, n_dp)
    greet_all(n_dp, n_ctx)
    gate_src = lambda peer: gate_ref.at[lax.rem(peer, n_ctx)]
    ins, outs = (rows_ref, grad_ref), (out_rows, out_grad)

    def gate_start(i, carry):
        spread_copy(n_dp, n_ctx, i, gate_src, out_gate, gate_send, gate_recv, True).start()
        return carry

    lax.fori_loop(1, n, gate_start, 0)

    def place(a, slot):
        return outs[a].at[:, pl.ds(pl.multiple_of(slot * cap, 8), cap)]

    def ring(a, k, sending):
        peer = lax.rem(c + k, n_ctx)
        owner = c if sending else lax.rem(c + n_ctx - k, n_ctx)
        return pltpu.make_async_remote_copy(
            src_ref=ins[a].at[peer],
            dst_ref=place(a, d * n_ctx + owner),
            send_sem=ring_send.at[a, k],
            recv_sem=ring_recv.at[a, k],
            device_id=(d, peer),
            device_id_type=MESH,
        )

    def forward(a, src, slot, to, send_sem, recv_sem, index):
        return pltpu.make_async_remote_copy(
            src_ref=src,
            dst_ref=place(a, slot),
            send_sem=send_sem.at[a, index],
            recv_sem=recv_sem.at[a, index],
            device_id=(to, c),
            device_id_type=MESH,
        )

    def slot_of(row, k):
        return row * n_ctx + lax.rem(c + n_ctx - k, n_ctx)

    loads = []
    for a in range(2):
        load = pltpu.make_async_copy(ins[a].at[c], own.at[a], own_sem.at[a])
        load.start()
        loads.append(load)
    for a in range(2):

        def ring_start(k, carry, a=a):
            ring(a, k, True).start()
            return carry

        lax.fori_loop(1, n_ctx, ring_start, 0)
    wloads = [
        pltpu.make_async_copy(ref, weights.at[i], weight_sem.at[i])
        for i, ref in enumerate((wg_ref, wu_ref))
    ] + [pltpu.make_async_copy(wd_ref, down_held, weight_sem.at[2])]
    for load in wloads:
        load.start()
    stores = []
    for a in range(2):
        loads[a].wait()
        store = pltpu.make_async_copy(own.at[a], place(a, me), own_sem.at[a])
        store.start()
        stores.append(store)
    out_gate[pl.ds(me, 1)] = gate_ref[pl.ds(c, 1)]

    def near_copies(a, k, first):
        slot = slot_of(d, k)
        src = ins[a].at[c] if first else place(a, slot)
        return (
            forward(a, src, slot, far, far_send, far_recv, k),
            forward(a, src, slot, sib, sib_send, sib_recv, k),
        )

    def sib_copy(a, k):
        slot = slot_of(far, k)
        return forward(a, place(a, slot), slot, sib, sib_send, sib_recv, n_ctx + k)

    def await_far(a, k):
        slot = slot_of(far, k)
        forward(a, place(a, slot), slot, far, far_send, far_recv, k).wait_recv()

    def await_sib(a):
        def wait(k, carry):
            slot = slot_of(sib, k)
            forward(a, place(a, slot), slot, sib, sib_send, sib_recv, k).wait_recv()
            slot = slot_of(far_sib, k)
            forward(a, place(a, slot), slot, sib, sib_send, sib_recv, n_ctx + k).wait_recv()
            return carry

        lax.fori_loop(0, n_ctx, wait, 0)

    def step(a, k):
        @pl.when(k < n_ctx)
        def _():
            ring(a, k, False).wait_recv()
            for copy in near_copies(a, k, False):
                copy.start()

        await_far(a, k - 1)
        sib_copy(a, k - 1).start()

    def chunk_at(u):
        q = lax.div(u, local)
        row = lax.rem(d + lax.div(q, 2) * (sib - d) + 2 * lax.rem(q, 2), n_dp)
        return lax.rem(u, local), pl.ds(pl.multiple_of(row * span, 8), span)

    def chunk_load(a, u):
        return pltpu.make_async_copy(
            outs[a].at[chunk_at(u)],
            chunk.at[lax.rem(u, 2)],
            chunk_sem.at[lax.rem(u, 2)],
        )

    def chunk_out(u, i):
        return pltpu.make_async_copy(
            pre.at[i, u],
            (out_pre_g, out_pre_u, out_down)[i].at[chunk_at(u)],
            pre_sem.at[i, u],
        )

    def compute(u, carry):
        chunk_load(0, u).wait()

        @pl.when(u + 1 < chunks)
        def _():
            chunk_load(0, u + 1).start()

        held = chunk[lax.rem(u, 2)]
        for i in range(2):
            pre[i, u] = jnp.dot(
                held, weights[i, lax.rem(u, local)], preferred_element_type=jnp.float32
            )
            chunk_out(u, i).start()
        return carry

    def compute_down(u, carry):
        chunk_load(1, u).wait()

        @pl.when(u + 1 < chunks)
        def _():
            chunk_load(1, u + 1).start()

        pre[2, u] = lax.dot_general(
            chunk[lax.rem(u, 2)],
            down_held[lax.rem(u, local)],
            (((1,), (1,)), ((), ())),
            preferred_element_type=jnp.float32,
        )
        chunk_out(u, 2).start()
        return carry

    def first(k, carry):
        step(0, k)
        return carry

    for copy in near_copies(0, 0, True):
        copy.start()
    lax.fori_loop(1, n_ctx + 1, first, 0)
    for copy in near_copies(1, 0, True):
        copy.start()
    stores[0].wait()
    await_sib(0)
    for load in wloads:
        load.wait()
    chunk_load(0, 0).start()

    def second(k, carry):
        step(1, k)
        lax.fori_loop(lax.div((k - 1) * chunks, n_ctx), lax.div(k * chunks, n_ctx), compute, 0)
        return carry

    lax.fori_loop(1, n_ctx + 1, second, 0)
    await_sib(1)
    stores[1].wait()
    chunk_load(1, 0).start()
    lax.fori_loop(0, chunks, compute_down, 0)
    for a in range(2):
        for copy in near_copies(a, 0, True):
            copy.wait_send()
        sib_copy(a, 0).wait_send()

        def drain(k, carry, a=a):
            ring(a, k, True).wait_send()
            for copy in near_copies(a, k, False):
                copy.wait_send()
            sib_copy(a, k).wait_send()
            return carry

        lax.fori_loop(1, n_ctx, drain, 0)

    def pre_finish(u, carry):
        for i in range(3):
            chunk_out(u, i).wait()
        return carry

    lax.fori_loop(0, chunks, pre_finish, 0)

    def gate_finish(i, carry):
        spread_copy(n_dp, n_ctx, i, gate_src, out_gate, gate_send, gate_recv, True).wait_send()
        spread_copy(n_dp, n_ctx, i, gate_src, out_gate, gate_send, gate_recv, False).wait_recv()
        return carry

    lax.fori_loop(1, n, gate_finish, 0)


def dispatch_rows(rows, grad, gate, gate_weight, up_weight, down_weight, n_dp, n_ctx):
    n = n_dp * n_ctx
    _, local, cap, width = rows.shape
    hidden = gate_weight.shape[2]
    arrived = jax.ShapeDtypeStruct((local, n * cap, width), rows.dtype)
    pre = jax.ShapeDtypeStruct((local, n * cap, hidden), jnp.float32)
    return pl.pallas_call(
        functools.partial(dispatch_kernel, n_dp, n_ctx, cap),
        out_shape=(arrived, arrived, jax.ShapeDtypeStruct((n, 8, 128), jnp.float32))
        + (pre,) * 3,
        in_specs=[ANY, ANY, VMEM, ANY, ANY, ANY],
        out_specs=(ANY, ANY, VMEM, ANY, ANY, ANY),
        scratch_shapes=[
            pltpu.VMEM((2, local, cap, width), rows.dtype),
            pltpu.VMEM((2,) + gate_weight.shape, gate_weight.dtype),
            pltpu.VMEM(down_weight.shape, down_weight.dtype),
            pltpu.VMEM((2, n_ctx * cap, width), rows.dtype),
            pltpu.VMEM((3, local * n_dp, n_ctx * cap, hidden), jnp.float32),
            pltpu.SemaphoreType.DMA((2,)),
            pltpu.SemaphoreType.DMA((3,)),
            pltpu.SemaphoreType.DMA((2,)),
            pltpu.SemaphoreType.DMA((3, local * n_dp)),
            pltpu.SemaphoreType.DMA((n,)),
            pltpu.SemaphoreType.DMA((n,)),
            pltpu.SemaphoreType.DMA((2, n_ctx)),
            pltpu.SemaphoreType.DMA((2, n_ctx)),
            pltpu.SemaphoreType.DMA((2, n_ctx)),
            pltpu.SemaphoreType.DMA((2, n_ctx)),
            pltpu.SemaphoreType.DMA((2, 2 * n_ctx)),
            pltpu.SemaphoreType.DMA((2, 2 * n_ctx)),
        ],
        compiler_params=pltpu.CompilerParams(
            collective_id=0, has_side_effects=True, vmem_limit_bytes=48 * 1024 * 1024
        ),
    )(rows, grad, gate, gate_weight, up_weight, down_weight)


def return_kernel(
    n_dp, n_ctx, cap, tile, back_ref, rows_ref, grad_ref, pg_ref, pu_ref, hid_ref, score_ref,
    out_ref, gate_out, up_out, down_out, out_score,
    mine, sib_land, far_out, far_land, done, pair, hid_raw, hid, row_tile, grad_tile, both, down,
    mine_sem, sib_send, sib_recv, far_send, far_recv, ring_send, ring_recv, own_sem,
    hold_sem, tile_sem, result_sem, score_send, score_recv,
):
    d, c = lax.axis_index("dp"), lax.axis_index("ctx")
    local = back_ref.shape[0]
    width, depth = rows_ref.shape[2], pg_ref.shape[2]
    across = width // tile
    units = local * across
    far = lax.rem(d + 2, n_dp)
    sib = d + 1 - 2 * lax.rem(d, 2)
    far_sib = lax.rem(sib + 2, n_dp)
    greet_all(n_dp, n_ctx)

    def dest(k):
        return lax.rem(c + k, n_ctx)

    def block(slot):
        return back_ref.at[:, pl.ds(pl.multiple_of(slot * cap, 8), cap)]

    def to_sib(k, which):
        row = far_sib if which == 0 else sib
        return pltpu.make_async_remote_copy(
            src_ref=block(row * n_ctx + dest(k)),
            dst_ref=sib_land.at[k, which],
            send_sem=sib_send.at[k, which],
            recv_sem=sib_recv.at[k, which],
            device_id=(sib, c),
            device_id_type=MESH,
        )

    def load(k, which):
        row = far if which == 0 else d
        return pltpu.make_async_copy(
            block(row * n_ctx + dest(k)), mine.at[k, which], mine_sem.at[k, which]
        )

    def to_far(k):
        return pltpu.make_async_remote_copy(
            src_ref=far_out.at[k],
            dst_ref=far_land.at[k],
            send_sem=far_send.at[k],
            recv_sem=far_recv.at[k],
            device_id=(far, c),
            device_id_type=MESH,
        )

    def ring(k, sending):
        owner = c if sending else lax.rem(c + n_ctx - k, n_ctx)
        return pltpu.make_async_remote_copy(
            src_ref=done.at[k],
            dst_ref=out_ref.at[owner],
            send_sem=ring_send.at[k],
            recv_sem=ring_recv.at[k],
            device_id=(d, dest(k)),
            device_id_type=MESH,
        )

    gaps = n_ctx + 1

    def turn(i):
        return lax.rem(i + 1, n_ctx)

    def tile_loads(u):
        e, slot = lax.div(u, across), lax.rem(u, 2)
        columns = pl.ds(pl.multiple_of(lax.rem(u, across) * tile, tile), tile)
        return (
            pltpu.make_async_copy(
                rows_ref.at[e, :, columns], row_tile.at[slot], tile_sem.at[0, slot]
            ),
            pltpu.make_async_copy(
                grad_ref.at[e, :, columns], grad_tile.at[slot], tile_sem.at[1, slot]
            ),
        )

    def results(u):
        e = lax.div(u, across)
        columns = pl.ds(pl.multiple_of(lax.rem(u, across) * tile, tile), tile)
        return (
            pltpu.make_async_copy(
                both.at[u, :, pl.ds(0, depth)], gate_out.at[e, columns], result_sem.at[0, u]
            ),
            pltpu.make_async_copy(
                both.at[u, :, pl.ds(depth, depth)], up_out.at[e, columns], result_sem.at[1, u]
            ),
            pltpu.make_async_copy(down.at[u], down_out.at[e, :, columns], result_sem.at[2, u]),
        )

    def unit(u, carry):
        for copy in tile_loads(u):
            copy.wait()

        @pl.when(u + 1 < units)
        def _():
            for copy in tile_loads(u + 1):
                copy.start()

        e, slot = lax.div(u, across), lax.rem(u, 2)
        both[u] = jnp.dot(
            row_tile[slot].T, pair[e], preferred_element_type=jnp.float32
        ).astype(jnp.bfloat16)
        down[u] = jnp.dot(
            hid[e], grad_tile[slot], preferred_element_type=jnp.float32
        ).astype(jnp.bfloat16)
        for copy in results(u):
            copy.start()
        return carry

    n = n_dp * n_ctx
    me = d * n_ctx + c
    score_src = lambda peer: score_ref.at[peer]

    def score_start(i, carry):
        spread_copy(n_dp, n_ctx, i, score_src, out_score, score_send, score_recv, True).start()
        return carry

    def score_finish(i, carry):
        spread_copy(n_dp, n_ctx, i, score_src, out_score, score_send, score_recv, True).wait_send()
        spread_copy(n_dp, n_ctx, i, score_src, out_score, score_send, score_recv, False).wait_recv()
        return carry

    def begin(i, carry):
        k = turn(i)
        for which in range(2):
            to_sib(k, which).start()
            load(k, which).start()
        return carry

    lax.fori_loop(0, n_ctx, begin, 0)
    holds = (
        pltpu.make_async_copy(pg_ref, pair.at[:, :, pl.ds(0, depth)], hold_sem.at[0]),
        pltpu.make_async_copy(pu_ref, pair.at[:, :, pl.ds(depth, depth)], hold_sem.at[1]),
        pltpu.make_async_copy(hid_ref, hid_raw, hold_sem.at[2]),
    )
    for copy in holds:
        copy.start()
    for copy in tile_loads(0):
        copy.start()

    def outward(i, carry):
        k = turn(i)
        to_sib(k, 0).wait_recv()
        load(k, 0).wait()
        far_out[k] = (
            mine[k, 0].astype(jnp.float32) + sib_land[k, 0].astype(jnp.float32)
        ).astype(jnp.bfloat16)
        to_far(k).start()
        return carry

    lax.fori_loop(0, n_ctx, outward, 0)
    lax.fori_loop(1, n, score_start, 0)
    out_score[pl.ds(me, 1)] = score_ref[pl.ds(me, 1)]
    for copy in holds:
        copy.wait()
    for e in range(local):
        hid[e] = hid_raw[e].T

    def inward(i, carry):
        k = turn(i)
        lax.fori_loop(lax.div(i * units, gaps), lax.div((i + 1) * units, gaps), unit, 0)
        to_sib(k, 1).wait_recv()
        load(k, 1).wait()
        to_far(k).wait_recv()
        done[k] = (
            mine[k, 1].astype(jnp.float32)
            + sib_land[k, 1].astype(jnp.float32)
            + far_land[k].astype(jnp.float32)
        ).astype(jnp.bfloat16)

        @pl.when(k > 0)
        def _():
            ring(k, True).start()

        return carry

    lax.fori_loop(0, n_ctx, inward, 0)
    own = pltpu.make_async_copy(done.at[0], out_ref.at[c], own_sem)
    own.start()
    lax.fori_loop(n_ctx * units // gaps, units, unit, 0)
    own.wait()
    lax.fori_loop(1, n, score_finish, 0)

    def drain(k, carry):
        to_sib(k, 0).wait_send()
        to_sib(k, 1).wait_send()
        to_far(k).wait_send()

        @pl.when(k > 0)
        def _():
            ring(k, True).wait_send()
            ring(k, False).wait_recv()

        return carry

    lax.fori_loop(0, n_ctx, drain, 0)

    def store_wait(u, carry):
        for copy in results(u):
            copy.wait()
        return carry

    lax.fori_loop(0, units, store_wait, 0)


def return_rows(back, rows, grad, pre_gate, pre_up, hidden, score, n_dp, n_ctx):
    local, total, width = back.shape
    cap = total // (n_dp * n_ctx)
    depth = pre_gate.shape[2]
    tile = 256 if width % 256 == 0 else 128
    units = local * (width // tile)
    block = (local, cap, width)
    low = back.dtype
    return pl.pallas_call(
        functools.partial(return_kernel, n_dp, n_ctx, cap, tile),
        out_shape=(
            jax.ShapeDtypeStruct((n_ctx,) + block, low),
            jax.ShapeDtypeStruct((local, width, depth), low),
            jax.ShapeDtypeStruct((local, width, depth), low),
            jax.ShapeDtypeStruct((local, depth, width), low),
            jax.ShapeDtypeStruct((n_dp * n_ctx, 8, 128), jnp.float32),
        ),
        in_specs=[ANY] * 6 + [VMEM],
        out_specs=(ANY,) * 4 + (VMEM,),
        scratch_shapes=[
            pltpu.VMEM((n_ctx, 2) + block, low),
            pltpu.VMEM((n_ctx, 2) + block, low),
            pltpu.VMEM((n_ctx,) + block, low),
            pltpu.VMEM((n_ctx,) + block, low),
            pltpu.VMEM((n_ctx,) + block, low),
            pltpu.VMEM((local, total, 2 * depth), low),
            pltpu.VMEM((local, total, depth), low),
            pltpu.VMEM((local, depth, total), low),
            pltpu.VMEM((2, total, tile), low),
            pltpu.VMEM((2, total, tile), low),
            pltpu.VMEM((units, tile, 2 * depth), low),
            pltpu.VMEM((units, depth, tile), low),
            pltpu.SemaphoreType.DMA((n_ctx, 2)),
            pltpu.SemaphoreType.DMA((n_ctx, 2)),
            pltpu.SemaphoreType.DMA((n_ctx, 2)),
            pltpu.SemaphoreType.DMA((n_ctx,)),
            pltpu.SemaphoreType.DMA((n_ctx,)),
            pltpu.SemaphoreType.DMA((n_ctx,)),
            pltpu.SemaphoreType.DMA((n_ctx,)),
            pltpu.SemaphoreType.DMA,
            pltpu.SemaphoreType.DMA((3,)),
            pltpu.SemaphoreType.DMA((2, 2)),
            pltpu.SemaphoreType.DMA((3, units)),
            pltpu.SemaphoreType.DMA((n_dp * n_ctx,)),
            pltpu.SemaphoreType.DMA((n_dp * n_ctx,)),
        ],
        compiler_params=pltpu.CompilerParams(
            collective_id=1, has_side_effects=True, vmem_limit_bytes=60 * 1024 * 1024
        ),
    )(back, rows, grad, pre_gate, pre_up, hidden, score)


def expert_pass(gate_pre, up_pre, grad_out, weight, gate_weight, up_weight):
    squash = jax.nn.sigmoid(SWISH_SCALE * gate_pre)
    full = gate_pre * squash * (up_pre + 1.0)
    hidden = full.astype(jnp.bfloat16)
    hidden_scaled = (weight[:, :, None] * full).astype(jnp.bfloat16)
    score = jnp.sum(grad_out * hidden.astype(jnp.float32), axis=2)
    grad_hidden = weight[:, :, None] * grad_out
    slope = squash + SWISH_SCALE * gate_pre * squash * (1.0 - squash)
    grad_pre_gate = (grad_hidden * (up_pre + 1.0) * slope).astype(jnp.bfloat16)
    grad_pre_up = (grad_hidden * gate_pre * squash).astype(jnp.bfloat16)
    back = jnp.einsum(
        "prf,pdf->prd", grad_pre_gate, gate_weight, preferred_element_type=jnp.float32
    )
    back = back + jnp.einsum(
        "prf,pdf->prd", grad_pre_up, up_weight, preferred_element_type=jnp.float32
    )
    return (grad_pre_gate, grad_pre_up, hidden_scaled, back.astype(jnp.bfloat16), score)


def tiles(x):
    return jnp.pad(x, ((0, 0), (0, 1024 - x.shape[1]))).reshape(x.shape[0], 8, 128)


def body(
    tokens, cotangent, expert_ids, norm_gain, router_weight, gate_weight, up_weight, down_weight
):
    n_ctx = lax.axis_size("ctx")
    n_dp = lax.axis_size("dp")
    n = n_dp * n_ctx
    local = gate_weight.shape[0]
    experts = router_weight.shape[1]
    rows_here = tokens.shape[0]
    picks = expert_ids.shape[1]
    width = tokens.shape[1]
    assigned = rows_here * picks
    capacity = max(2, rows_here * picks * 5 // (4 * experts))
    capacity = -(-capacity // 8) * 8
    slots = experts * capacity
    widened = tokens.astype(jnp.float32)
    inverse = lax.rsqrt(jnp.mean(widened * widened, axis=1, keepdims=True) + EPSILON)
    scaled = widened * inverse
    normed = (scaled * norm_gain).astype(jnp.bfloat16)
    logits = jnp.dot(normed, router_weight, preferred_element_type=jnp.float32)
    labels = jnp.arange(experts, dtype=jnp.int32)
    member = expert_ids[:, :, None] == labels
    chosen = jnp.sum(jnp.where(member, logits[:, None, :], 0.0), axis=2)
    lifted = jnp.exp(chosen)
    gates = lifted / jnp.sum(lifted, axis=1, keepdims=True)
    hits = member.reshape(assigned, experts).astype(jnp.int32)
    rank = jnp.sum((jnp.cumsum(hits, axis=0) - 1) * hits, axis=1)
    position = expert_ids.reshape(-1) * capacity + rank
    match = (jnp.arange(slots, dtype=jnp.int32)[:, None] == position[None, :]).astype(jnp.float32)
    dispatch = jnp.sum(match.reshape(slots, rows_here, picks), axis=2)
    dispatch_low = dispatch.astype(jnp.bfloat16)
    out_rows = jnp.dot(dispatch_low, normed, preferred_element_type=jnp.float32).astype(
        jnp.bfloat16
    )
    out_rows = out_rows.reshape(n_ctx, local, capacity, width)
    out_grad = jnp.dot(dispatch_low, cotangent, preferred_element_type=jnp.float32).astype(
        jnp.bfloat16
    )
    out_grad = out_grad.reshape(n_ctx, local, capacity, width)
    out_gate = jnp.dot(match, gates.reshape(-1), precision=lax.Precision.HIGHEST)
    out_gate = tiles(out_gate.reshape(n_ctx, local * capacity))
    rows, upstream, weight, gate_pre, up_pre, grad_out = dispatch_rows(
        out_rows, out_grad, out_gate, gate_weight, up_weight, down_weight, n_dp, n_ctx
    )
    weight = weight.reshape(n, 1024)[:, : local * capacity].reshape(n, local, capacity)
    weight = weight.transpose(1, 0, 2).reshape(local, n * capacity)
    pre_gate, pre_up, hidden, back, score = expert_pass(
        gate_pre, up_pre, grad_out, weight, gate_weight, up_weight
    )
    score_out = score.reshape(local, n, capacity).transpose(1, 0, 2).reshape(n, local * capacity)
    back_slots, gate_grad, up_grad, down_grad, score_parts = return_rows(
        back, rows, upstream, pre_gate, pre_up, hidden, tiles(score_out), n_dp, n_ctx
    )
    score_slots = jnp.sum(score_parts.reshape(n_dp, n_ctx, 8, 128), axis=0)
    back_flat = back_slots.reshape(slots, width)
    score_flat = score_slots.reshape(n_ctx, 1024)[:, : local * capacity].reshape(slots)
    grad_tok = jnp.dot(dispatch_low.T, back_flat, preferred_element_type=jnp.float32)
    score_tok = jnp.dot(score_flat, match, precision=lax.Precision.HIGHEST).reshape(
        rows_here, picks
    )
    mixed = jnp.sum(gates * score_tok, axis=1, keepdims=True)
    grad_chosen = gates * (score_tok - mixed)
    grad_logits = jnp.sum(jnp.where(member, grad_chosen[:, :, None], 0.0), axis=1).astype(
        jnp.bfloat16
    )
    grad_normed = grad_tok + jnp.dot(
        grad_logits, router_weight.T, preferred_element_type=jnp.float32
    )
    router_part = jnp.dot(normed.T, grad_logits, preferred_element_type=jnp.float32)
    gain_part = jnp.sum(grad_normed * scaled, axis=0)
    share = width // n
    parts = jnp.concatenate(
        [router_part.reshape(n, share * experts), gain_part.reshape(n, share)], axis=1
    )
    sums = exchange(tiles(parts), n_dp, n_ctx, 1, 3).reshape(1024)
    router_grad = sums[: share * experts].reshape(share, experts)
    gain_grad = sums[share * experts : share * experts + share]
    grad_scaled = grad_normed * norm_gain
    correction = jnp.mean(grad_scaled * scaled, axis=1, keepdims=True)
    grad_input = (
        cotangent.astype(jnp.float32) + inverse * (grad_scaled - scaled * correction)
    ).astype(jnp.bfloat16)
    return (grad_input, gate_grad, up_grad, down_grad, router_grad, gain_grad)


def solution(mesh):
    return jax.shard_map(
        body,
        mesh=mesh,
        in_specs=(
            P(("dp", "ctx"), None),
            P(("dp", "ctx"), None),
            P(("dp", "ctx"), None),
            P(),
            P(),
            P("ctx", None, "dp"),
            P("ctx", None, "dp"),
            P("ctx", "dp", None),
        ),
        out_specs=(
            P(("dp", "ctx"), None),
            P("ctx", None, "dp"),
            P("ctx", None, "dp"),
            P("ctx", "dp", None),
            P(("dp", "ctx"), None),
            P(("dp", "ctx")),
        ),
        check_vma=False,
    )
```
